8 devices in a mesh: rep: 2 (over y, z), dp: 4 (over x, core).
Axes of the slice: x: 2, y: 2, z: 1, core: 2. Of those that a mesh axis runs over, the one named last changes fastest.
Arguments:
- a: bfloat16 [8, 4, 4096, 896], P(('rep', 'dp')), parts along dimension 0
- g: bfloat16 [8, 4, 4096, 2304], P(('rep', 'dp')), parts along dimension 0
Outputs:
- output: bfloat16 [8, 896, 2304], P('rep'), parts along dimension 0
There are 2 independent parts. The reference program is written for one: setup_inputs(seed, part) draws one part's arguments, and reference() takes and returns one part's arrays. A program takes and returns all parts, laid end to end along the dimension named above; each array names one.
All inputs are finite; a program needn't handle non-finite values.
Results may differ from the reference program's by a relative error of at most 0.012.
Values are sent between devices in bfloat16 or wider.
A program may use at most 2 GiB of HBM per device.

```python
import jax
import jax.numpy as jnp
from jax import lax

DEVICES = 4
MATRICES = 4
TOKENS = 4096
D = 896
FF = 2304


def setup_inputs(seed: int = 0, part: int = 0) -> dict:
    ka, kg, ks = (jax.random.fold_in(k, part) for k in jax.random.split(jax.random.key(seed), 3))
    size = 2.0 ** jax.random.uniform(ks, (DEVICES, MATRICES, 1, 1), jnp.float32, -1.0, 1.0)
    a = jax.random.normal(ka, (DEVICES, MATRICES, TOKENS, D), jnp.float32)
    g = size * jax.random.normal(kg, (DEVICES, MATRICES, TOKENS, FF), jnp.float32) * (DEVICES * TOKENS) ** -0.5
    return {"a": a.astype(jnp.bfloat16), "g": g.astype(jnp.bfloat16)}


def reference(a, g):
    def take(so_far, one):
        return so_far + jnp.einsum("ntd,ntf->ndf", *one, preferred_element_type=jnp.float32), None

    return lax.scan(take, jnp.zeros((MATRICES, D, FF), jnp.float32), (a, g))[0].astype(jnp.bfloat16)
```

```python
import jax
import jax.numpy as jnp
from jax import lax
from jax.experimental import pallas as pl
from jax.experimental.pallas import tpu as pltpu
from jax.sharding import PartitionSpec as P

MESH = pl.DeviceIdType.MESH
COLS = 256
STRIP = 128
G_SLOTS = 3
LAG = 2


def kernel(
    a_ref, g_ref, out_ref,
    at, raw, gs, p_send, acc, s_own, s_recv,
    a_sem, g_sem, ps_sem, p0_sem, pr_sem, xs_sem, xr_sem, rs_sem, rr_sem,
):
    n_mat, rows, cols = out_ref.shape
    half = rows // 2
    per = cols // COLS
    panels = n_mat * per
    strips = rows // STRIP

    me = lax.axis_index("dp")
    core = lax.rem(me, 2)
    sibling = me + 1 - 2 * core
    peer = lax.rem(me + 2, 4)
    own = pl.multiple_of(core * half, half)
    other = pl.multiple_of((1 - core) * half, half)

    def load_strip(n, r, slot):
        c = pl.multiple_of(r * STRIP, STRIP)
        return pltpu.make_async_copy(a_ref.at[0, n, :, pl.ds(c, STRIP)], raw.at[slot], a_sem.at[slot])

    def load_panel(p):
        c = pl.multiple_of(lax.rem(p, per) * COLS, COLS)
        slot = lax.rem(p, G_SLOTS)
        return pltpu.make_async_copy(g_ref.at[0, p // per, :, pl.ds(c, COLS)], gs.at[slot], g_sem.at[slot])

    def tile(p, first, size):
        c = pl.multiple_of(lax.rem(p, per) * COLS, COLS)
        return out_ref.at[p // per, pl.ds(first, size), pl.ds(c, COLS)]

    def send_partial(p, lo, size, recv):
        slot = lax.rem(p, 2)
        return pltpu.make_async_remote_copy(
            src_ref=p_send.at[slot, pl.ds(lo, size)], dst_ref=tile(p, other + lo, size),
            send_sem=ps_sem.at[slot], recv_sem=recv,
            device_id={"dp": sibling}, device_id_type=MESH)

    def recv_partial(p, lo, size, recv):
        return pltpu.make_async_remote_copy(
            src_ref=p_send.at[0, pl.ds(lo, size)], dst_ref=tile(p, own + lo, size),
            send_sem=ps_sem.at[0], recv_sem=recv,
            device_id={"dp": sibling}, device_id_type=MESH)

    def exchange(p, lo, size):
        return pltpu.make_async_remote_copy(
            src_ref=s_own.at[p, pl.ds(lo, size)], dst_ref=s_recv.at[p, pl.ds(lo, size)],
            send_sem=xs_sem, recv_sem=xr_sem.at[p],
            device_id={"dp": peer}, device_id_type=MESH)

    def forward(p):
        return pltpu.make_async_remote_copy(
            src_ref=tile(p, own, half), dst_ref=tile(p, own, half),
            send_sem=rs_sem, recv_sem=rr_sem,
            device_id={"dp": sibling}, device_id_type=MESH)

    def dot(first, size, slot):
        return lax.dot_general(
            at[pl.ds(first, size)], gs[slot], (((1,), (0,)), ((), ())), preferred_element_type=jnp.float32)

    def chip_sum(p, lo, size):
        got = tile(p, own + lo, size)[...].astype(jnp.float32)
        s_own[p, pl.ds(lo, size)] = (acc[pl.ds(lo, size)] + got).astype(s_own.dtype)

    def combine(p):
        exchange(p, 0, half).wait_recv()
        both = s_own[p].astype(jnp.float32) + s_recv[p].astype(jnp.float32)
        tile(p, own, half)[...] = both.astype(out_ref.dtype)
        forward(p).start()

    def flip(r):
        load_strip(0, r, r).wait()
        at[pl.ds(pl.multiple_of(r * STRIP, STRIP), STRIP)] = raw[r].T

    order = []
    for i in range(strips // 2):
        order += [(1 - core) * (strips // 2 + 1) + i, core * (strips // 2 + 1) + i]
    load_strip(0, order[0], order[0]).start()
    load_panel(0).start()
    load_strip(0, order[1], order[1]).start()
    for r in order[2:] + [strips // 2]:
        load_strip(0, r, r).start()
    for p in range(1, G_SLOTS):
        load_panel(p).start()

    barrier = pltpu.get_barrier_semaphore()
    for d in (sibling, peer):
        pl.semaphore_signal(barrier, inc=1, device_id={"dp": d}, device_id_type=MESH)
    pl.semaphore_wait(barrier, 2)

    blocks = [(i * STRIP, STRIP) for i in range(strips // 2)] + [(strips // 2 * STRIP, STRIP // 2)]

    def place(h, i):
        lo, size = blocks[i]
        if i == len(blocks) - 1:
            lo = (1 - h) * lo
        else:
            lo = lo + h * (STRIP // 2)
        return pl.multiple_of(h * half + lo, STRIP // 2), pl.multiple_of(lo, STRIP // 2), size

    def first(i):
        if i < len(blocks) - 1:
            flip(order[2 * i])
        else:
            flip(strips // 2)
        row, lo, size = place(1 - core, i)
        if i == 0:
            load_panel(0).wait()
        p_send[0, pl.ds(lo, size)] = dot(row, size, 0).astype(p_send.dtype)
        send_partial(0, lo, size, p0_sem.at[i]).start()

    def second(i):
        if i < len(blocks) - 1:
            flip(order[2 * i + 1])
        row, lo, size = place(core, i)
        acc[pl.ds(lo, size)] = dot(row, size, 0)

    def third(i):
        _, lo, size = place(core, i)
        recv_partial(0, lo, size, p0_sem.at[i]).wait_recv()
        chip_sum(0, lo, size)
        exchange(0, lo, size).start()

    first(0)
    for i in range(len(blocks)):
        second(i)
        if i + 1 < len(blocks):
            first(i + 1)
        third(i)
    load_panel(G_SLOTS).start()

    def step(p, carry):
        n, j = p // per, lax.rem(p, per)
        slot, ps = lax.rem(p, G_SLOTS), lax.rem(p, 2)

        @pl.when(j == 0)
        def _():
            def turn(r, c):
                flip(r)
                return c

            lax.fori_loop(0, strips, turn, 0)

        @pl.when((j == 1) & (n < n_mat - 1))
        def _():
            def more(r, c):
                load_strip(n + 1, r, r).start()
                return c

            lax.fori_loop(0, strips, more, 0)

        load_panel(p).wait()

        @pl.when(p >= 2)
        def _():
            send_partial(p - 2, 0, half, pr_sem.at[p - 2]).wait_send()

        p_send[ps] = dot(other, half, slot).astype(p_send.dtype)

        @pl.when(p >= 2)
        def _():
            recv_partial(p - 1, 0, half, pr_sem.at[p - 1]).wait_recv()
            chip_sum(p - 1, 0, half)

        send_partial(p, 0, half, pr_sem.at[p]).start()
        acc[...] = dot(own, half, slot)

        @pl.when(p >= 2)
        def _():
            exchange(p - 1, 0, half).start()

        @pl.when(p + G_SLOTS < panels)
        def _():
            load_panel(p + G_SLOTS).start()

        @pl.when(p >= LAG + 1)
        def _():
            combine(p - 1 - LAG)

        return carry

    lax.fori_loop(1, panels, step, 0)

    last = panels - 1
    recv_partial(last, 0, half, pr_sem.at[last]).wait_recv()
    chip_sum(last, 0, half)
    exchange(last, 0, half).start()

    def drain(p, carry):
        combine(p)
        return carry

    lax.fori_loop(last - LAG, panels, drain, 0)

    for p in (last - 1, last):
        send_partial(p, 0, half, pr_sem.at[p]).wait_send()

    def everything(send, recv):
        return pltpu.make_async_remote_copy(
            src_ref=s_own, dst_ref=s_recv, send_sem=send, recv_sem=recv,
            device_id={"dp": sibling}, device_id_type=MESH)

    everything(xs_sem, rr_sem).wait_send()
    everything(rs_sem, rr_sem).wait()


def solution(mesh):
    def sums(a, g):
        _, n, tokens, d = a.shape
        ff = g.shape[-1]
        half, panels, strips = d // 2, n * ff // COLS, d // STRIP
        dma = pltpu.SemaphoreType.DMA
        return pl.pallas_call(
            kernel,
            out_shape=pltpu.VMEM((n, d, ff), jnp.bfloat16),
            in_specs=[pl.BlockSpec(memory_space=pl.ANY)] * 2,
            out_specs=pl.BlockSpec(memory_space=pltpu.VMEM),
            scratch_shapes=[
                pltpu.VMEM((d, tokens), jnp.bfloat16),
                pltpu.VMEM((strips, tokens, STRIP), jnp.bfloat16),
                pltpu.VMEM((G_SLOTS, tokens, COLS), jnp.bfloat16),
                pltpu.VMEM((2, half, COLS), jnp.bfloat16),
                pltpu.VMEM((half, COLS), jnp.float32),
                pltpu.VMEM((panels, half, COLS), jnp.bfloat16),
                pltpu.VMEM((panels, half, COLS), jnp.bfloat16),
                dma((strips,)), dma((G_SLOTS,)), dma((2,)), dma((4,)), dma((panels,)),
                dma, dma((panels,)), dma, dma,
            ],
            compiler_params=pltpu.CompilerParams(
                collective_id=0, has_side_effects=True, vmem_limit_bytes=46 * 1024 * 1024
            ),
            name="sums",
        )(a, g)

    return jax.shard_map(
        sums, mesh=mesh, in_specs=(P(("rep", "dp")),) * 2, out_specs=P("rep"), check_vma=False
    )
```

```python
import jax
import jax.numpy as jnp
from jax import lax
from jax.experimental import pallas as pl
from jax.experimental.pallas import tpu as pltpu
from jax.sharding import PartitionSpec as P

MESH = pl.DeviceIdType.MESH
COLS = 256
STRIP = 128
G_SLOTS = 3
LAG = 4


def kernel(
    a_ref, g_ref, out_ref,
    at, raw, gs, p_send, acc, s_own, s_recv,
    a_sem, g_sem, ps_sem, p0_sem, pr_sem, xs_sem, xr_sem, rs_sem, rr_sem,
):
    n_mat, rows, cols = out_ref.shape
    half = rows // 2
    size = half // 2
    per = cols // COLS
    panels = n_mat * per
    strips = rows // STRIP
    pairs = strips // 2
    rest = STRIP // 2

    me = lax.axis_index("dp")
    core = lax.rem(me, 2)
    sibling = me + 1 - 2 * core
    peer = lax.rem(me + 2, 4)
    own = pl.multiple_of(core * half, half)
    other = pl.multiple_of((1 - core) * half, half)

    def load_strip(n, r, slot):
        c = pl.multiple_of(r * STRIP, STRIP)
        return pltpu.make_async_copy(a_ref.at[0, n, :, pl.ds(c, STRIP)], raw.at[slot], a_sem.at[slot])

    def load_panel(p):
        c = pl.multiple_of(lax.rem(p, per) * COLS, COLS)
        slot = lax.rem(p, G_SLOTS)
        return pltpu.make_async_copy(g_ref.at[0, p // per, :, pl.ds(c, COLS)], gs.at[slot], g_sem.at[slot])

    def tile(p, first, n):
        c = pl.multiple_of(lax.rem(p, per) * COLS, COLS)
        return out_ref.at[p // per, pl.ds(first, n), pl.ds(c, COLS)]

    def remote(src, dst, send, recv, to):
        return pltpu.make_async_remote_copy(
            src_ref=src, dst_ref=dst, send_sem=send, recv_sem=recv,
            device_id={"dp": to}, device_id_type=MESH)

    def exchange(p, lo, n, recv):
        return remote(s_own.at[p, pl.ds(lo, n)], s_recv.at[p, pl.ds(lo, n)], xs_sem, recv, peer)

    def chip_sum(p, lo, n, mine):
        got = tile(p, own + lo, n)[...].astype(jnp.float32)
        s_own[p, pl.ds(lo, n)] = (mine[...] + got).astype(s_own.dtype)

    def flip(r):
        load_strip(0, r, r).wait()
        at[pl.ds(pl.multiple_of(r * STRIP, STRIP), STRIP)] = raw[r].T

    def dot(first, n, slot):
        return lax.dot_general(
            at[pl.ds(first, n)], gs[slot], (((1,), (0,)), ((), ())), preferred_element_type=jnp.float32)

    def strip(k):
        h = core + (1 - 2 * core) * (1 - lax.rem(k, 2))
        mid = k // (2 * pairs)
        return (1 - mid) * (h * (pairs + 1) + k // 2) + mid * pairs, h

    def lower(h, i):
        return pl.multiple_of(h * rest + i * STRIP, rest)

    load_strip(0, *[strip(0)[0]] * 2).start()
    load_panel(0).start()

    def load(k, c):
        load_strip(0, *[strip(k)[0]] * 2).start()
        return c

    lax.fori_loop(1, strips, load, 0)
    for p in range(1, G_SLOTS):
        load_panel(p).start()

    barrier = pltpu.get_barrier_semaphore()
    for d in (sibling, peer):
        pl.semaphore_signal(barrier, inc=1, device_id={"dp": d}, device_id_type=MESH)

    def send_strip(lo, n, i):
        return remote(p_send.at[0, pl.ds(lo, n)], tile(0, other + lo, n), ps_sem.at[0], p0_sem.at[i], sibling)

    def take_strip(lo, n, i):
        remote(p_send.at[0, pl.ds(lo, n)], tile(0, own + lo, n), ps_sem.at[0], p0_sem.at[i], sibling).wait_recv()
        chip_sum(0, lo, n, acc.at[pl.ds(lo, n)])
        exchange(0, lo, n, xr_sem.at[0]).start()

    flat = acc.at[pl.ds(half, STRIP)]

    def fill(k, carry):
        r, h = strip(k)
        i = k // 2
        flip(r)

        @pl.when(k == 0)
        def _():
            load_panel(0).wait()

        flat[...] = dot(pl.multiple_of(r * STRIP, STRIP), STRIP, 0)

        @pl.when((lax.rem(k, 2) == 0) & (k < 2 * pairs))
        def _():
            lo = lower(h, i)
            p_send[0, pl.ds(lo, STRIP)] = flat[...].astype(p_send.dtype)

            @pl.when(k == 0)
            def _():
                pl.semaphore_wait(barrier, 2)

            send_strip(lo, STRIP, i).start()

        @pl.when(lax.rem(k, 2) == 1)
        def _():
            acc[pl.ds(lower(h, i), STRIP)] = flat[...]

        @pl.when(k == 2 * pairs)
        def _():
            lo = pl.multiple_of(core * pairs * STRIP, rest)
            theirs = pl.multiple_of((1 - core) * rest, rest)
            p_send[0, pl.ds(lo, rest)] = flat[pl.ds(theirs, rest)].astype(p_send.dtype)
            send_strip(lo, rest, pairs).start()
            mine = pl.multiple_of(core * rest, rest)
            acc[pl.ds(pl.multiple_of((1 - core) * pairs * STRIP, rest), rest)] = flat[pl.ds(mine, rest)]

        @pl.when((lax.rem(k, 2) == 0) & (k >= 2))
        def _():
            take_strip(lower(core, i - 1), STRIP, i - 1)

        return carry

    lax.fori_loop(0, strips, fill, 0)
    take_strip(pl.multiple_of((1 - core) * pairs * STRIP, rest), rest, pairs)
    load_panel(G_SLOTS).start()

    def spot(k):
        return k // 2, pl.multiple_of(lax.rem(k, 2) * size, size)

    def send_partial(k):
        p, lo = spot(k)
        slot = lax.rem(k, 2)
        return remote(p_send.at[slot, pl.ds(0, size)], tile(p, other + lo, size), ps_sem.at[slot], pr_sem.at[k], sibling)

    def finish(k):
        p, lo = spot(k)
        remote(p_send.at[0, pl.ds(0, size)], tile(p, own + lo, size), ps_sem.at[0], pr_sem.at[k], sibling).wait_recv()
        chip_sum(p, lo, size, acc.at[pl.ds(size, size)])

    def leave(k):
        p, lo = spot(k)
        return exchange(p, lo, size, xr_sem.at[k])

    def combine(k):
        @pl.when(k == 1)
        def _():
            exchange(0, 0, half, xr_sem.at[0]).wait_recv()

        @pl.when(k > 1)
        def _():
            leave(k).wait_recv()

        def one(k, c):
            p, lo = spot(k)
            both = s_own[p, pl.ds(lo, size)].astype(jnp.float32) + s_recv[p, pl.ds(lo, size)].astype(jnp.float32)
            here = tile(p, own + lo, size)
            here[...] = both.astype(out_ref.dtype)
            remote(here, here, rs_sem, rr_sem, sibling).start()
            return c

        lax.fori_loop(k - 1 // k, k + 1, one, 0)

    def step(q, carry):
        k, t = q // 2, lax.rem(q, 2)
        p, b = k // 2, lax.rem(k, 2)
        n, j = p // per, lax.rem(p, per)

        @pl.when((b == 0) & (t == 0))
        def _():
            load_panel(p).wait()

            @pl.when(j == 0)
            def _():
                def turn(r, c):
                    flip(r)
                    return c

                lax.fori_loop(0, strips, turn, 0)

            @pl.when((j == 1) & (n < n_mat - 1))
            def _():
                def more(r, c):
                    load_strip(n + 1, r, r).start()
                    return c

                lax.fori_loop(0, strips, more, 0)

        h = core + (1 - 2 * core) * (1 - t)
        acc[pl.ds(pl.multiple_of(t * size, size), size)] = dot(
            pl.multiple_of((2 * h + b) * size, size), size, lax.rem(p, G_SLOTS))

        @pl.when(t == 0)
        def _():
            @pl.when(k == 2)
            def _():
                send_strip(0, half, 0).wait_send()

            @pl.when(k >= 4)
            def _():
                send_partial(k - 2).wait_send()

            p_send[lax.rem(k, 2), pl.ds(0, size)] = acc[pl.ds(0, size)].astype(p_send.dtype)

        @pl.when((t == 0) & (k >= 3))
        def _():
            finish(k - 1)

        @pl.when(t == 0)
        def _():
            send_partial(k).start()

        @pl.when((t == 0) & (k >= 3))
        def _():
            leave(k - 1).start()

        @pl.when((t == 1) & (b == 1) & (p + G_SLOTS < panels))
        def _():
            load_panel(p + G_SLOTS).start()

        @pl.when((t == 1) & (k - 1 - LAG >= 1))
        def _():
            combine(k - 1 - LAG)

        return carry

    lax.fori_loop(4, 4 * panels, step, 0)

    last = 2 * panels - 1
    finish(last)
    leave(last).start()

    def drain(k, carry):
        combine(k)
        return carry

    lax.fori_loop(last - LAG, last + 1, drain, 0)

    for k in (last - 1, last):
        send_partial(k).wait_send()

    remote(s_own, s_recv, xs_sem, rr_sem, peer).wait_send()
    remote(s_own, s_recv, rs_sem, rr_sem, sibling).wait()


def solution(mesh):
    def sums(a, g):
        _, n, tokens, d = a.shape
        ff = g.shape[-1]
        half, panels, strips = d // 2, n * ff // COLS, d // STRIP
        dma = pltpu.SemaphoreType.DMA
        return pl.pallas_call(
            kernel,
            out_shape=pltpu.VMEM((n, d, ff), jnp.bfloat16),
            in_specs=[pl.BlockSpec(memory_space=pl.ANY)] * 2,
            out_specs=pl.BlockSpec(memory_space=pltpu.VMEM),
            scratch_shapes=[
                pltpu.VMEM((d, tokens), jnp.bfloat16),
                pltpu.VMEM((strips, tokens, STRIP), jnp.bfloat16),
                pltpu.VMEM((G_SLOTS, tokens, COLS), jnp.bfloat16),
                pltpu.VMEM((2, half, COLS), jnp.bfloat16),
                pltpu.VMEM((half + STRIP, COLS), jnp.float32),
                pltpu.VMEM((panels, half, COLS), jnp.bfloat16),
                pltpu.VMEM((panels, half, COLS), jnp.bfloat16),
                dma((strips,)), dma((G_SLOTS,)), dma((2,)), dma((strips // 2 + 1,)), dma((2 * panels,)),
                dma, dma((2 * panels,)), dma, dma,
            ],
            compiler_params=pltpu.CompilerParams(
                collective_id=0, has_side_effects=True, vmem_limit_bytes=46 * 1024 * 1024
            ),
            name="sums",
        )(a, g)

    return jax.shard_map(
        sums, mesh=mesh, in_specs=(P(("rep", "dp")),) * 2, out_specs=P("rep"), check_vma=False
    )
```

```python
import jax
import jax.numpy as jnp
from jax import lax
from jax.experimental import pallas as pl
from jax.experimental.pallas import tpu as pltpu
from jax.sharding import PartitionSpec as P

MESH = pl.DeviceIdType.MESH
COLS = 256
STRIP = 128
G_SLOTS = 3
LAG = 4
P_RING = 4
X_RING = 12


def kernel(
    a_ref, g_ref, out_ref,
    at, raw, gs, p_send, acc, s_own, s_recv,
    a_sem, g_sem, ps_sem, p0_sem, pr_sem, xs_sem, xr_sem, rs_sem, rr_sem,
):
    n_mat, rows, cols = out_ref.shape
    half = rows // 2
    size = half // 2
    per = cols // COLS
    panels = n_mat * per
    strips = rows // STRIP
    pairs = strips // 2
    rest = STRIP // 2

    me = lax.axis_index("dp")
    core = lax.rem(me, 2)
    sibling = me + 1 - 2 * core
    peer = lax.rem(me + 2, 4)
    own = pl.multiple_of(core * half, half)
    other = pl.multiple_of((1 - core) * half, half)

    def load_strip(n, r, slot):
        c = pl.multiple_of(r * STRIP, STRIP)
        return pltpu.make_async_copy(a_ref.at[0, n, :, pl.ds(c, STRIP)], raw.at[slot], a_sem.at[slot])

    def load_panel(p):
        c = pl.multiple_of(lax.rem(p, per) * COLS, COLS)
        slot = lax.rem(p, G_SLOTS)
        return pltpu.make_async_copy(g_ref.at[0, p // per, :, pl.ds(c, COLS)], gs.at[slot], g_sem.at[slot])

    def tile(p, first, n):
        c = pl.multiple_of(lax.rem(p, per) * COLS, COLS)
        return out_ref.at[p // per, pl.ds(first, n), pl.ds(c, COLS)]

    def remote(src, dst, send, recv, to):
        return pltpu.make_async_remote_copy(
            src_ref=src, dst_ref=dst, send_sem=send, recv_sem=recv,
            device_id={"dp": to}, device_id_type=MESH)

    def exchange(p, lo, n, recv):
        return remote(s_own.at[p, pl.ds(lo, n)], s_recv.at[p, pl.ds(lo, n)], xs_sem, recv, peer)

    def chip_sum(p, lo, n, mine):
        got = tile(p, own + lo, n)[...].astype(jnp.float32)
        s_own[p, pl.ds(lo, n)] = (mine[...] + got).astype(s_own.dtype)

    def flip(r):
        at[pl.ds(pl.multiple_of(r * STRIP, STRIP), STRIP)] = raw[r].T

    def dot(first, n, slot):
        return lax.dot_general(
            at[pl.ds(first, n)], gs[slot], (((1,), (0,)), ((), ())), preferred_element_type=jnp.float32)

    def strip(k):
        h = core + (1 - 2 * core) * (1 - lax.rem(k, 2))
        mid = k // (2 * pairs)
        return (1 - mid) * (h * (pairs + 1) + k // 2) + mid * pairs, h

    def lower(h, i):
        return pl.multiple_of(h * rest + i * STRIP, rest)

    load_strip(0, *[strip(0)[0]] * 2).start()
    load_panel(0).start()

    def load(k, c):
        load_strip(0, *[strip(k)[0]] * 2).start()
        return c

    lax.fori_loop(1, strips, load, 0)
    for p in range(1, G_SLOTS):
        load_panel(p).start()

    barrier = pltpu.get_barrier_semaphore()
    for d in (sibling, peer):
        pl.semaphore_signal(barrier, inc=1, device_id={"dp": d}, device_id_type=MESH)

    def send_strip(lo, n, i):
        return remote(p_send.at[0, pl.ds(lo, n)], tile(0, other + lo, n), ps_sem.at[0], p0_sem.at[i], sibling)

    def take_strip(lo, n, i):
        remote(p_send.at[0, pl.ds(lo, n)], tile(0, own + lo, n), ps_sem.at[0], p0_sem.at[i], sibling).wait_recv()
        chip_sum(0, lo, n, acc.at[pl.ds(lo, n)])
        exchange(0, lo, n, xr_sem.at[0]).start()

    flat = acc.at[pl.ds(half, STRIP)]

    def fill(k, carry):
        r, h = strip(k)
        i = k // 2

        @pl.when(k == 0)
        def _():
            load_panel(0).wait()

        load_strip(0, r, r).wait()
        flip(r)
        flat[...] = dot(pl.multiple_of(r * STRIP, STRIP), STRIP, 0)

        @pl.when((lax.rem(k, 2) == 0) & (k < 2 * pairs))
        def _():
            lo = lower(h, i)
            p_send[0, pl.ds(lo, STRIP)] = flat[...].astype(p_send.dtype)

            @pl.when(k == 0)
            def _():
                pl.semaphore_wait(barrier, 2)

            send_strip(lo, STRIP, i).start()

        @pl.when(lax.rem(k, 2) == 1)
        def _():
            acc[pl.ds(lower(h, i), STRIP)] = flat[...]

        @pl.when(k == 2 * pairs)
        def _():
            lo = pl.multiple_of(core * pairs * STRIP, rest)
            theirs = pl.multiple_of((1 - core) * rest, rest)
            p_send[0, pl.ds(lo, rest)] = flat[pl.ds(theirs, rest)].astype(p_send.dtype)
            send_strip(lo, rest, pairs).start()
            mine = pl.multiple_of(core * rest, rest)
            acc[pl.ds(pl.multiple_of((1 - core) * pairs * STRIP, rest), rest)] = flat[pl.ds(mine, rest)]

        @pl.when((lax.rem(k, 2) == 0) & (k >= 2))
        def _():
            take_strip(lower(core, i - 1), STRIP, i - 1)

        return carry

    lax.fori_loop(0, strips, fill, 0)
    take_strip(pl.multiple_of((1 - core) * pairs * STRIP, rest), rest, pairs)
    load_panel(G_SLOTS).start()

    def spot(k):
        return k // 2, pl.multiple_of(lax.rem(k, 2) * size, size)

    def send_partial(k):
        p, lo = spot(k)
        slot = lax.rem(k, 2)
        return remote(p_send.at[slot, pl.ds(0, size)], tile(p, other + lo, size), ps_sem.at[slot], pr_sem.at[lax.rem(k, P_RING)], sibling)

    def finish(k):
        p, lo = spot(k)
        remote(p_send.at[0, pl.ds(0, size)], tile(p, own + lo, size), ps_sem.at[0], pr_sem.at[lax.rem(k, P_RING)], sibling).wait_recv()
        chip_sum(p, lo, size, acc.at[pl.ds(size, size)])

    def leave(k):
        p, lo = spot(k)
        return exchange(p, lo, size, xr_sem.at[lax.rem(k, X_RING)])

    def combine(k):
        @pl.when(k == 1)
        def _():
            exchange(0, 0, half, xr_sem.at[0]).wait_recv()

        @pl.when(k > 1)
        def _():
            leave(k).wait_recv()

        def one(k, c):
            p, lo = spot(k)
            both = s_own[p, pl.ds(lo, size)].astype(jnp.float32) + s_recv[p, pl.ds(lo, size)].astype(jnp.float32)
            here = tile(p, own + lo, size)
            here[...] = both.astype(out_ref.dtype)
            remote(here, here, rs_sem, rr_sem, sibling).start()
            return c

        lax.fori_loop(k - 1 // k, k + 1, one, 0)

    def step(q, carry):
        k, t = q // 2, lax.rem(q, 2)
        p, b = k // 2, lax.rem(k, 2)
        n, j = p // per, lax.rem(p, per)

        @pl.when((b == 0) & (t == 0))
        def _():
            load_panel(p).wait()

            @pl.when(j == 0)
            def _():
                def turn(r, c):
                    load_strip(0, r, r).wait()
                    flip(r)
                    return c

                lax.fori_loop(0, strips, turn, 0)

            @pl.when((j == 1) & (n < n_mat - 1))
            def _():
                def more(r, c):
                    load_strip(n + 1, r, r).start()
                    return c

                lax.fori_loop(0, strips, more, 0)

        h = core + (1 - 2 * core) * (1 - t)
        acc[pl.ds(pl.multiple_of(t * size, size), size)] = dot(
            pl.multiple_of((2 * h + b) * size, size), size, lax.rem(p, G_SLOTS))

        @pl.when(t == 0)
        def _():
            @pl.when(k == 2)
            def _():
                send_strip(0, half, 0).wait_send()

            @pl.when(k >= 4)
            def _():
                send_partial(k - 2).wait_send()

            p_send[lax.rem(k, 2), pl.ds(0, size)] = acc[pl.ds(0, size)].astype(p_send.dtype)

        @pl.when((t == 0) & (k >= 3))
        def _():
            finish(k - 1)

        @pl.when(t == 0)
        def _():
            send_partial(k).start()

        @pl.when((t == 0) & (k >= 3))
        def _():
            leave(k - 1).start()

        @pl.when((t == 1) & (b == 1) & (p + G_SLOTS < panels))
        def _():
            load_panel(p + G_SLOTS).start()

        @pl.when((t == 1) & (k - 1 - LAG >= 1))
        def _():
            combine(k - 1 - LAG)

        return carry

    lax.fori_loop(4, 4 * panels, step, 0)

    last = 2 * panels - 1
    finish(last)
    leave(last).start()

    def drain(k, carry):
        combine(k)
        return carry

    lax.fori_loop(last - LAG, last + 1, drain, 0)

    for k in (last - 1, last):
        send_partial(k).wait_send()

    remote(s_own, s_recv, xs_sem, rr_sem, peer).wait_send()
    remote(s_own, s_recv, rs_sem, rr_sem, sibling).wait()


def solution(mesh):
    def sums(a, g):
        _, n, tokens, d = a.shape
        ff = g.shape[-1]
        half, panels, strips = d // 2, n * ff // COLS, d // STRIP
        dma = pltpu.SemaphoreType.DMA
        return pl.pallas_call(
            kernel,
            out_shape=pltpu.VMEM((n, d, ff), jnp.bfloat16),
            in_specs=[pl.BlockSpec(memory_space=pl.ANY)] * 2,
            out_specs=pl.BlockSpec(memory_space=pltpu.VMEM),
            scratch_shapes=[
                pltpu.VMEM((d, tokens), jnp.bfloat16),
                pltpu.VMEM((strips, tokens, STRIP), jnp.bfloat16),
                pltpu.VMEM((G_SLOTS, tokens, COLS), jnp.bfloat16),
                pltpu.VMEM((2, half, COLS), jnp.bfloat16),
                pltpu.VMEM((half + STRIP, COLS), jnp.float32),
                pltpu.VMEM((panels, half, COLS), jnp.bfloat16),
                pltpu.VMEM((panels, half, COLS), jnp.bfloat16),
                dma((strips,)), dma((G_SLOTS,)), dma((2,)), dma((strips // 2 + 1,)), dma((P_RING,)),
                dma, dma((X_RING,)), dma, dma,
            ],
            compiler_params=pltpu.CompilerParams(
                collective_id=0, has_side_effects=True, vmem_limit_bytes=46 * 1024 * 1024
            ),
            name="sums",
        )(a, g)

    return jax.shard_map(
        sums, mesh=mesh, in_specs=(P(("rep", "dp")),) * 2, out_specs=P("rep"), check_vma=False
    )
```

```python
import jax
import jax.numpy as jnp
from jax import lax
from jax.experimental import pallas as pl
from jax.experimental.pallas import tpu as pltpu
from jax.sharding import PartitionSpec as P


MESH = pl.DeviceIdType.MESH
COLS = 256
STRIP = 128
G_SLOTS = 3
LAG = 4
P_RING = 4
X_RING = 12
LATE = 2


def kernel(
    a_ref, g_ref, out_ref, turn_mine, turn_other, turn_got, late_mine, late_other,
    at, raw, gs, p_send, acc, s_own, s_recv,
    a_sem, g_sem, ps_sem, p0_sem, pr_sem, xs_sem, xr_sem, rs_sem, rr_sem,
):
    n_mat, rows, cols = out_ref.shape
    half = rows // 2
    size = half // 2
    per = cols // COLS
    panels = n_mat * per
    early = 2 * panels - LATE - 1
    strips = rows // STRIP
    pairs = strips // 2
    rest = STRIP // 2

    me = lax.axis_index("dp")
    core = lax.rem(me, 2)
    sibling = me + 1 - 2 * core
    peer = lax.rem(me + 2, 4)
    own = pl.multiple_of(core * half, half)
    other = pl.multiple_of((1 - core) * half, half)

    def load_strip(n, r, slot):
        c = pl.multiple_of(r * STRIP, STRIP)
        return pltpu.make_async_copy(a_ref.at[0, n, :, pl.ds(c, STRIP)], raw.at[slot], a_sem.at[slot])

    def load_panel(p):
        c = pl.multiple_of(lax.rem(p, per) * COLS, COLS)
        slot = lax.rem(p, G_SLOTS)
        return pltpu.make_async_copy(g_ref.at[0, p // per, :, pl.ds(c, COLS)], gs.at[slot], g_sem.at[slot])

    def tile(p, first, n):
        c = pl.multiple_of(lax.rem(p, per) * COLS, COLS)
        return out_ref.at[p // per, pl.ds(first, n), pl.ds(c, COLS)]

    def remote(src, dst, send, recv, to):
        return pltpu.make_async_remote_copy(
            src_ref=src, dst_ref=dst, send_sem=send, recv_sem=recv,
            device_id={"dp": to}, device_id_type=MESH)

    def exchange(p, lo, n, recv):
        return remote(s_own.at[p, pl.ds(lo, n)], s_recv.at[p, pl.ds(lo, n)], xs_sem, recv, peer)

    def chip_sum(p, lo, n, mine):
        got = tile(p, own + lo, n)[...].astype(jnp.float32)
        s_own[p, pl.ds(lo, n)] = (mine[...] + got).astype(s_own.dtype)

    def flip(r):
        at[pl.ds(pl.multiple_of(r * STRIP, STRIP), STRIP)] = raw[r].T

    def dot(first, n, slot):
        return lax.dot_general(
            at[pl.ds(first, n)], gs[slot], (((1,), (0,)), ((), ())), preferred_element_type=jnp.float32)

    def strip(k):
        h = core + (1 - 2 * core) * (1 - lax.rem(k, 2))
        mid = k // (2 * pairs)
        return (1 - mid) * (h * (pairs + 1) + k // 2) + mid * pairs, h

    def lower(h, i):
        return pl.multiple_of(h * rest + i * STRIP, rest)

    load_strip(0, *[strip(0)[0]] * 2).start()
    load_panel(0).start()

    def load(k, c):
        load_strip(0, *[strip(k)[0]] * 2).start()
        return c

    lax.fori_loop(1, strips, load, 0)
    for p in range(1, G_SLOTS):
        load_panel(p).start()

    barrier = pltpu.get_barrier_semaphore()
    for d in (sibling, peer):
        pl.semaphore_signal(barrier, inc=1, device_id={"dp": d}, device_id_type=MESH)

    def send_strip(lo, n, i):
        return remote(p_send.at[0, pl.ds(lo, n)], tile(0, other + lo, n), ps_sem.at[0], p0_sem.at[i], sibling)

    def take_strip(lo, n, i):
        remote(p_send.at[0, pl.ds(lo, n)], tile(0, own + lo, n), ps_sem.at[0], p0_sem.at[i], sibling).wait_recv()
        chip_sum(0, lo, n, acc.at[pl.ds(lo, n)])
        exchange(0, lo, n, xr_sem.at[0]).start()

    flat = acc.at[pl.ds(half, STRIP)]

    def fill(k, carry):
        r, h = strip(k)
        i = k // 2

        @pl.when(k == 0)
        def _():
            load_panel(0).wait()

        load_strip(0, r, r).wait()
        flip(r)
        flat[...] = dot(pl.multiple_of(r * STRIP, STRIP), STRIP, 0)

        @pl.when((lax.rem(k, 2) == 0) & (k < 2 * pairs))
        def _():
            lo = lower(h, i)
            p_send[0, pl.ds(lo, STRIP)] = flat[...].astype(p_send.dtype)

            @pl.when(k == 0)
            def _():
                pl.semaphore_wait(barrier, 2)

            send_strip(lo, STRIP, i).start()

        @pl.when(lax.rem(k, 2) == 1)
        def _():
            acc[pl.ds(lower(h, i), STRIP)] = flat[...]

        @pl.when(k == 2 * pairs)
        def _():
            lo = pl.multiple_of(core * pairs * STRIP, rest)
            theirs = pl.multiple_of((1 - core) * rest, rest)
            p_send[0, pl.ds(lo, rest)] = flat[pl.ds(theirs, rest)].astype(p_send.dtype)
            send_strip(lo, rest, pairs).start()
            mine = pl.multiple_of(core * rest, rest)
            acc[pl.ds(pl.multiple_of((1 - core) * pairs * STRIP, rest), rest)] = flat[pl.ds(mine, rest)]

        @pl.when((lax.rem(k, 2) == 0) & (k >= 2))
        def _():
            take_strip(lower(core, i - 1), STRIP, i - 1)

        return carry

    lax.fori_loop(0, strips, fill, 0)
    take_strip(pl.multiple_of((1 - core) * pairs * STRIP, rest), rest, pairs)
    load_panel(G_SLOTS).start()

    def spot(k):
        return k // 2, pl.multiple_of(lax.rem(k, 2) * size, size)

    def send_partial(k):
        p, lo = spot(k)
        slot = lax.rem(k, 2)
        return remote(p_send.at[slot, pl.ds(0, size)], tile(p, other + lo, size), ps_sem.at[slot], pr_sem.at[lax.rem(k, P_RING)], sibling)

    def finish(k):
        p, lo = spot(k)
        remote(p_send.at[0, pl.ds(0, size)], tile(p, own + lo, size), ps_sem.at[0], pr_sem.at[lax.rem(k, P_RING)], sibling).wait_recv()
        chip_sum(p, lo, size, acc.at[pl.ds(size, size)])

        @pl.when(k == early)
        def _():
            turn_mine[0] = s_own[p, pl.ds(lo, size)]
            remote(turn_mine, turn_other, rs_sem, rr_sem, sibling).start()

        @pl.when(k > early)
        def _():
            i = k - early - 1
            late_mine[i] = s_own[p, pl.ds(lo, size)]
            remote(late_mine.at[i], late_other.at[i], rs_sem, rr_sem, sibling).start()

    def leave(k):
        p, lo = spot(k)
        return exchange(p, lo, size, xr_sem.at[lax.rem(k, X_RING)])

    def leave_unfinished():
        p, lo = early // 2, early % 2 * size
        return remote(s_own.at[p, pl.ds(lo, size)], turn_got.at[0], xs_sem, xr_sem.at[early % X_RING], peer)

    def combine(k):
        @pl.when(k == 1)
        def _():
            exchange(0, 0, half, xr_sem.at[0]).wait_recv()

        @pl.when(k > 1)
        def _():
            leave(k).wait_recv()

        def one(k, c):
            p, lo = spot(k)
            both = s_own[p, pl.ds(lo, size)].astype(jnp.float32) + s_recv[p, pl.ds(lo, size)].astype(jnp.float32)
            here = tile(p, own + lo, size)
            here[...] = both.astype(out_ref.dtype)
            remote(here, here, rs_sem, rr_sem, sibling).start()
            return c

        lax.fori_loop(k - 1 // k, k + 1, one, 0)

    def step(q, carry):
        k, t = q // 2, lax.rem(q, 2)
        p, b = k // 2, lax.rem(k, 2)
        n, j = p // per, lax.rem(p, per)

        @pl.when((b == 0) & (t == 0))
        def _():
            load_panel(p).wait()

            @pl.when(j == 0)
            def _():
                def turn(r, c):
                    load_strip(0, r, r).wait()
                    flip(r)
                    return c

                lax.fori_loop(0, strips, turn, 0)

            @pl.when((j == 1) & (n < n_mat - 1))
            def _():
                def more(r, c):
                    load_strip(n + 1, r, r).start()
                    return c

                lax.fori_loop(0, strips, more, 0)

        h = core + (1 - 2 * core) * (1 - t)
        acc[pl.ds(pl.multiple_of(t * size, size), size)] = dot(
            pl.multiple_of((2 * h + b) * size, size), size, lax.rem(p, G_SLOTS))

        @pl.when(t == 0)
        def _():
            @pl.when(k == 2)
            def _():
                send_strip(0, half, 0).wait_send()

            @pl.when(k >= 4)
            def _():
                send_partial(k - 2).wait_send()

            p_send[lax.rem(k, 2), pl.ds(0, size)] = acc[pl.ds(0, size)].astype(p_send.dtype)

        @pl.when((t == 0) & (k >= 3))
        def _():
            finish(k - 1)

        @pl.when(t == 0)
        def _():
            send_partial(k).start()

        @pl.when((t == 0) & (k >= 3) & (k <= early))
        def _():
            leave(k - 1).start()

        @pl.when((t == 0) & (k == early + 1))
        def _():
            leave_unfinished().start()

        @pl.when((t == 1) & (b == 1) & (p + G_SLOTS < panels))
        def _():
            load_panel(p + G_SLOTS).start()

        @pl.when((t == 1) & (k - 1 - LAG >= 1))
        def _():
            combine(k - 1 - LAG)

        return carry

    lax.fori_loop(4, 4 * panels, step, 0)

    last = 2 * panels - 1
    finish(last)

    def drain(k, carry):
        combine(k)
        return carry

    lax.fori_loop(last - LAG, early, drain, 0)

    for k in (last - 1, last):
        send_partial(k).wait_send()

    full = (early + 1) // 2
    remote(s_own.at[pl.ds(0, full)], s_recv.at[pl.ds(0, full)], xs_sem, rr_sem, peer).wait_send()
    if early % 2 == 0:
        exchange(full, 0, size, rr_sem).wait_send()
    remote(s_own, s_recv, rs_sem, rr_sem, sibling).wait()
    leave_unfinished().wait_recv()


def copy_out(x_ref, o_ref, sem):
    n, rows, _ = x_ref.shape
    size = rows // 4
    copies = []
    for i in range(n):
        for j in range(4):
            part = (i, pl.ds(j * size, size))
            copies.append(pltpu.make_async_copy(x_ref.at[part], o_ref.at[part], sem.at[i, j]))
    for c in copies:
        c.start()
    for c in copies:
        c.wait()


def add_late(so_far, *refs):
    *terms, o_ref, buf, sem = refs
    n_mat, rows, cols = o_ref.shape
    size = rows // 4
    per = cols // COLS
    core = lax.rem(lax.axis_index("dp"), 2)
    copies = []
    for i in range(LATE + 1):
        k = 2 * n_mat * per - LATE - 1 + i
        p, b = divmod(k, 2)
        n, j = divmod(p, per)
        group, at = terms[4 * min(i, 1) :][:4], max(i - 1, 0)
        for h in range(2):
            ours, theirs = group[h][at].astype(jnp.float32), group[2 + h][at].astype(jnp.float32)
            buf[h, i] = (ours + theirs).astype(buf.dtype)
            first = pl.multiple_of((core + (1 - 2 * core) * h) * 2 * size + b * size, size)
            there = o_ref.at[n, pl.ds(first, size), pl.ds(j * COLS, COLS)]
            copies.append(pltpu.make_async_copy(buf.at[h, i], there, sem.at[h, i]))
            copies[-1].start()
    for c in copies:
        c.wait()


def solution(mesh):
    def sums(a, g):
        _, n, tokens, d = a.shape
        ff = g.shape[-1]
        half, panels, strips = d // 2, n * ff // COLS, d // STRIP
        dma = pltpu.SemaphoreType.DMA
        block = (half // 2, COLS)
        turn, late = (pltpu.VMEM((i, *block), jnp.bfloat16) for i in (1, LATE))
        cross, across = [(0, 2), (2, 0), (1, 3), (3, 1)], [(0, 1), (1, 0), (2, 3), (3, 2)]
        vmem, hbm = pl.BlockSpec(memory_space=pltpu.VMEM), pl.BlockSpec(memory_space=pltpu.HBM)
        result = jax.ShapeDtypeStruct((n, d, ff), jnp.bfloat16)
        most, turn_mine, turn_other, turn_got, late_mine, late_other = pl.pallas_call(
            kernel,
            out_shape=(pltpu.VMEM((n, d, ff), jnp.bfloat16), turn, turn, turn, late, late),
            in_specs=[pl.BlockSpec(memory_space=pl.ANY)] * 2,
            out_specs=(vmem,) * 6,
            scratch_shapes=[
                pltpu.VMEM((d, tokens), jnp.bfloat16),
                pltpu.VMEM((strips, tokens, STRIP), jnp.bfloat16),
                pltpu.VMEM((G_SLOTS, tokens, COLS), jnp.bfloat16),
                pltpu.VMEM((2, half, COLS), jnp.bfloat16),
                pltpu.VMEM((half + STRIP, COLS), jnp.float32),
                pltpu.VMEM((panels, half, COLS), jnp.bfloat16),
                pltpu.VMEM((panels, half, COLS), jnp.bfloat16),
                dma((strips,)), dma((G_SLOTS,)), dma((2,)), dma((strips // 2 + 1,)), dma((P_RING,)),
                dma, dma((X_RING,)), dma, dma,
            ],
            compiler_params=pltpu.CompilerParams(
                collective_id=0, has_side_effects=True, vmem_limit_bytes=46 * 1024 * 1024
            ),
            name="sums",
        )(a, g)
        late_got = lax.ppermute(late_mine, "dp", cross)
        turn_got_other = lax.ppermute(turn_got, "dp", across)
        out = pl.pallas_call(
            copy_out,
            out_shape=result,
            in_specs=[vmem],
            out_specs=hbm,
            scratch_shapes=[dma((n, 4))],
            compiler_params=pltpu.CompilerParams(vmem_limit_bytes=1024 * 1024),
            cost_estimate=pl.CostEstimate(flops=10**10, bytes_accessed=2 * n * d * ff, transcendentals=0),
            name="copy_out",
        )(most)
        late_got_other = lax.ppermute(late_got, "dp", across)
        return pl.pallas_call(
            add_late,
            out_shape=result,
            in_specs=[hbm] + [vmem] * 8,
            out_specs=hbm,
            scratch_shapes=[pltpu.VMEM((2, LATE + 1, *block), jnp.bfloat16), dma((2, LATE + 1))],
            input_output_aliases={0: 0},
            compiler_params=pltpu.CompilerParams(vmem_limit_bytes=4 * 1024 * 1024),
            name="add_late",
        )(
            out,
            *(turn_mine, turn_other, turn_got, turn_got_other),
            *(late_mine, late_other, late_got, late_got_other),
        )

    return jax.shard_map(
        sums, mesh=mesh, in_specs=(P(("rep", "dp")),) * 2, out_specs=P("rep"), check_vma=False
    )
```

```python
import functools

import jax
import jax.numpy as jnp
from jax import lax
from jax.experimental import pallas as pl
from jax.experimental.pallas import tpu as pltpu
from jax.sharding import PartitionSpec as P


MESH = pl.DeviceIdType.MESH
COLS = 256
STRIP = 128
G_SLOTS = 3
LAG = 2
P_RING = 4
X_RING = 8
SPLIT = 4


def kernel(
    a_ref, g_ref, out_ref, turn_got, turn_mine, turn_other, late_mine, late_other,
    at, raw, gs, p_send, acc, s_own, s_recv,
    a_sem, g_sem, ps_sem, p0_sem, pr_sem, xs_sem, xr_sem, rs_sem, rr_sem,
):
    n_mat, rows, cols = out_ref.shape
    half = rows // 2
    size = half // 2
    per = cols // COLS
    panels = n_mat * per
    turn = panels - 2
    strips = rows // STRIP
    pairs = strips // 2
    rest = STRIP // 2

    me = lax.axis_index("dp")
    core = lax.rem(me, 2)
    sibling = me + 1 - 2 * core
    peer = lax.rem(me + 2, 4)
    own = pl.multiple_of(core * half, half)
    other = pl.multiple_of((1 - core) * half, half)

    def load_strip(n, r, slot):
        c = pl.multiple_of(r * STRIP, STRIP)
        return pltpu.make_async_copy(a_ref.at[0, n, :, pl.ds(c, STRIP)], raw.at[slot], a_sem.at[slot])

    def load_panel(p):
        c = pl.multiple_of(lax.rem(p, per) * COLS, COLS)
        slot = lax.rem(p, G_SLOTS)
        return pltpu.make_async_copy(g_ref.at[0, p // per, :, pl.ds(c, COLS)], gs.at[slot], g_sem.at[slot])

    def tile(p, first, n):
        c = pl.multiple_of(lax.rem(p, per) * COLS, COLS)
        return out_ref.at[p // per, pl.ds(first, n), pl.ds(c, COLS)]

    def remote(src, dst, send, recv, to):
        return pltpu.make_async_remote_copy(
            src_ref=src, dst_ref=dst, send_sem=send, recv_sem=recv,
            device_id={"dp": to}, device_id_type=MESH)

    def exchange(p, lo, n, recv):
        return remote(s_own.at[p, pl.ds(lo, n)], s_recv.at[p, pl.ds(lo, n)], xs_sem, recv, peer)

    def chip_sum(p, lo, n, mine):
        got = tile(p, own + lo, n)[...].astype(jnp.float32)
        s_own[p, pl.ds(lo, n)] = (mine[...] + got).astype(s_own.dtype)

    def flip(r):
        at[pl.ds(pl.multiple_of(r * STRIP, STRIP), STRIP)] = raw[r].T

    def dot(first, n, slot):
        return lax.dot_general(
            at[pl.ds(first, n)], gs[slot], (((1,), (0,)), ((), ())), preferred_element_type=jnp.float32)

    def strip(k):
        h = core + (1 - 2 * core) * (1 - lax.rem(k, 2))
        mid = k // (2 * pairs)
        return (1 - mid) * (h * (pairs + 1) + k // 2) + mid * pairs, h

    def lower(h, i):
        return pl.multiple_of(h * rest + i * STRIP, rest)

    load_strip(0, *[strip(0)[0]] * 2).start()
    load_panel(0).start()

    def load(k, c):
        load_strip(0, *[strip(k)[0]] * 2).start()
        return c

    lax.fori_loop(1, strips, load, 0)
    for p in range(1, G_SLOTS):
        load_panel(p).start()

    barrier = pltpu.get_barrier_semaphore()
    for d in (sibling, peer):
        pl.semaphore_signal(barrier, inc=1, device_id={"dp": d}, device_id_type=MESH)

    def send_strip(lo, n, i):
        return remote(p_send.at[0, pl.ds(lo, n)], tile(0, other + lo, n), ps_sem.at[0], p0_sem.at[i], sibling)

    def take_strip(lo, n, i):
        remote(p_send.at[0, pl.ds(lo, n)], tile(0, own + lo, n), ps_sem.at[0], p0_sem.at[i], sibling).wait_recv()
        chip_sum(0, lo, n, acc.at[pl.ds(lo, n)])
        exchange(0, lo, n, xr_sem.at[0]).start()

    flat = acc.at[pl.ds(half, STRIP)]

    def fill(k, carry):
        r, h = strip(k)
        i = k // 2

        @pl.when(k == 0)
        def _():
            load_panel(0).wait()

        load_strip(0, r, r).wait()
        flip(r)
        flat[...] = dot(pl.multiple_of(r * STRIP, STRIP), STRIP, 0)

        @pl.when((lax.rem(k, 2) == 0) & (k < 2 * pairs))
        def _():
            lo = lower(h, i)
            p_send[0, pl.ds(lo, STRIP)] = flat[...].astype(p_send.dtype)

            @pl.when(k == 0)
            def _():
                pl.semaphore_wait(barrier, 2)

            send_strip(lo, STRIP, i).start()

        @pl.when(lax.rem(k, 2) == 1)
        def _():
            acc[pl.ds(lower(h, i), STRIP)] = flat[...]

        @pl.when(k == 2 * pairs)
        def _():
            lo = pl.multiple_of(core * pairs * STRIP, rest)
            theirs = pl.multiple_of((1 - core) * rest, rest)
            p_send[0, pl.ds(lo, rest)] = flat[pl.ds(theirs, rest)].astype(p_send.dtype)
            send_strip(lo, rest, pairs).start()
            mine = pl.multiple_of(core * rest, rest)
            acc[pl.ds(pl.multiple_of((1 - core) * pairs * STRIP, rest), rest)] = flat[pl.ds(mine, rest)]

        @pl.when((lax.rem(k, 2) == 0) & (k >= 2))
        def _():
            take_strip(lower(core, i - 1), STRIP, i - 1)

        return carry

    lax.fori_loop(0, strips, fill, 0)
    take_strip(pl.multiple_of((1 - core) * pairs * STRIP, rest), rest, pairs)
    load_panel(G_SLOTS).start()

    def spot(k):
        return k // 2, pl.multiple_of(lax.rem(k, 2) * size, size)

    def send_partial(k):
        p, lo = spot(k)
        slot = lax.rem(k, 2)
        return remote(p_send.at[slot, pl.ds(0, size)], tile(p, other + lo, size), ps_sem.at[slot], pr_sem.at[lax.rem(k, P_RING)], sibling)

    def finish(k):
        p, lo = spot(k)
        remote(p_send.at[0, pl.ds(0, size)], tile(p, own + lo, size), ps_sem.at[0], pr_sem.at[lax.rem(k, P_RING)], sibling).wait_recv()
        chip_sum(p, lo, size, acc.at[pl.ds(size, size)])
        here = pl.ds(lo, size)
        for i, (mine, other) in enumerate(((turn_mine, turn_other), (late_mine, late_other))):

            @pl.when(p == turn + i)
            def _(mine=mine, other=other):
                mine[here] = s_own[p, here]
                remote(mine.at[here], other.at[here], rs_sem, rr_sem, sibling).start()

    def arrival(p):
        return xr_sem.at[lax.rem(p, X_RING)]

    def leave(k):
        p, lo = spot(k)

        @pl.when(p < SPLIT)
        def _():
            exchange(p, lo, size, arrival(p)).start()

        @pl.when((lo > 0) & (p >= SPLIT) & (p < turn))
        def _():
            exchange(p, 0, half, arrival(p)).start()

        @pl.when((lo > 0) & (p == turn))
        def _():
            leave_unfinished().start()

    def leave_unfinished():
        return remote(s_own.at[turn], turn_got, xs_sem, xr_sem.at[turn % X_RING], peer)

    def combine(p):
        exchange(p, 0, half, arrival(p)).wait_recv()

        def one(b, c):
            lo = pl.multiple_of(b * size, size)
            both = s_own[p, pl.ds(lo, size)].astype(jnp.float32) + s_recv[p, pl.ds(lo, size)].astype(jnp.float32)
            here = tile(p, own + lo, size)
            here[...] = both.astype(out_ref.dtype)
            remote(here, here, rs_sem, rr_sem, sibling).start()
            return c

        lax.fori_loop(0, 2, one, 0)

    def step(q, carry):
        k, t = q // 2, lax.rem(q, 2)
        p, b = k // 2, lax.rem(k, 2)
        n, j = p // per, lax.rem(p, per)

        @pl.when((b == 0) & (t == 0))
        def _():
            load_panel(p).wait()

            @pl.when(j == 0)
            def _():
                def turn(r, c):
                    load_strip(0, r, r).wait()
                    flip(r)
                    return c

                lax.fori_loop(0, strips, turn, 0)

            @pl.when((j == 1) & (n < n_mat - 1))
            def _():
                def more(r, c):
                    load_strip(n + 1, r, r).start()
                    return c

                lax.fori_loop(0, strips, more, 0)

        h = core + (1 - 2 * core) * (1 - t)
        acc[pl.ds(pl.multiple_of(t * size, size), size)] = dot(
            pl.multiple_of((2 * h + b) * size, size), size, lax.rem(p, G_SLOTS))

        @pl.when(t == 0)
        def _():
            @pl.when(k == 2)
            def _():
                send_strip(0, half, 0).wait_send()

            @pl.when(k >= 4)
            def _():
                send_partial(k - 2).wait_send()

            p_send[lax.rem(k, 2), pl.ds(0, size)] = acc[pl.ds(0, size)].astype(p_send.dtype)

        @pl.when(t == 0)
        def _():
            send_partial(k).start()

        @pl.when((t == 1) & (b == 1) & (p + G_SLOTS < panels))
        def _():
            load_panel(p + G_SLOTS).start()

        @pl.when(t == 1)
        def _():
            finish(k)
            leave(k)

        @pl.when((t == 1) & (b == 1) & (p >= LAG))
        def _():
            combine(p - LAG)

        return carry

    lax.fori_loop(4, 4 * panels, step, 0)

    def drain(p, carry):
        combine(p)
        return carry

    lax.fori_loop(panels - LAG, turn, drain, 0)

    for k in (2 * panels - 2, 2 * panels - 1):
        send_partial(k).wait_send()

    sent = pl.ds(0, turn + 1)
    remote(s_own.at[sent], s_recv.at[sent], xs_sem, rr_sem, peer).wait_send()
    remote(s_own, s_recv, rs_sem, rr_sem, sibling).wait()
    leave_unfinished().wait_recv()


def copy_out(x_ref, o_ref, sem):
    n, rows, _ = x_ref.shape
    size = rows // 4
    copies = []
    for i in range(n):
        for j in range(4):
            part = (i, pl.ds(j * size, size))
            copies.append(pltpu.make_async_copy(x_ref.at[part], o_ref.at[part], sem.at[i, j]))
    for c in copies:
        c.start()
    for c in copies:
        c.wait()


def add_panel(back, so_far, mine, got, other, got_other, o_ref, buf, sem):
    n_mat, rows, cols = o_ref.shape
    half = rows // 2
    per = cols // COLS
    n, j = divmod(n_mat * per - back, per)
    core = lax.rem(lax.axis_index("dp"), 2)
    copies = []
    for h, (ours, theirs) in enumerate(((mine, got), (other, got_other))):
        buf[h] = (ours[...].astype(jnp.float32) + theirs[...].astype(jnp.float32)).astype(buf.dtype)
        first = pl.multiple_of((core + (1 - 2 * core) * h) * half, half)
        there = o_ref.at[n, pl.ds(first, half), pl.ds(j * COLS, COLS)]
        copies.append(pltpu.make_async_copy(buf.at[h], there, sem.at[h]))
        copies[-1].start()
    for c in copies:
        c.wait()


def solution(mesh):
    def sums(a, g):
        _, n, tokens, d = a.shape
        ff = g.shape[-1]
        half, panels, strips = d // 2, n * ff // COLS, d // STRIP
        dma = pltpu.SemaphoreType.DMA
        block = (half, COLS)
        cross, across = [(0, 2), (2, 0), (1, 3), (3, 1)], [(0, 1), (1, 0), (2, 3), (3, 2)]
        vmem, hbm = pl.BlockSpec(memory_space=pltpu.VMEM), pl.BlockSpec(memory_space=pltpu.HBM)
        result = jax.ShapeDtypeStruct((n, d, ff), jnp.bfloat16)
        most, turn_got, turn_mine, turn_other, late_mine, late_other = pl.pallas_call(
            kernel,
            out_shape=(pltpu.VMEM((n, d, ff), jnp.bfloat16), *[pltpu.VMEM(block, jnp.bfloat16)] * 5),
            in_specs=[pl.BlockSpec(memory_space=pl.ANY)] * 2,
            out_specs=(vmem,) * 6,
            scratch_shapes=[
                pltpu.VMEM((d, tokens), jnp.bfloat16),
                pltpu.VMEM((strips, tokens, STRIP), jnp.bfloat16),
                pltpu.VMEM((G_SLOTS, tokens, COLS), jnp.bfloat16),
                pltpu.VMEM((2, half, COLS), jnp.bfloat16),
                pltpu.VMEM((half + STRIP, COLS), jnp.float32),
                pltpu.VMEM((panels, half, COLS), jnp.bfloat16),
                pltpu.VMEM((panels, half, COLS), jnp.bfloat16),
                dma((strips,)), dma((G_SLOTS,)), dma((2,)), dma((strips // 2 + 1,)), dma((P_RING,)),
                dma, dma((X_RING,)), dma, dma,
            ],
            compiler_params=pltpu.CompilerParams(
                collective_id=0, has_side_effects=True, vmem_limit_bytes=46 * 1024 * 1024
            ),
            name="sums",
        )(a, g)

        def add(back, out, *terms):
            return pl.pallas_call(
                functools.partial(add_panel, back),
                out_shape=result,
                in_specs=[hbm] + [vmem] * 4,
                out_specs=hbm,
                scratch_shapes=[pltpu.VMEM((2, *block), jnp.bfloat16), dma((2,))],
                input_output_aliases={0: 0},
                compiler_params=pltpu.CompilerParams(vmem_limit_bytes=4 * 1024 * 1024),
                name="add_panel",
            )(out, *terms)

        late_got = lax.ppermute(late_mine, "dp", cross)
        turn_got_other = lax.ppermute(turn_got, "dp", across)
        out = pl.pallas_call(
            copy_out,
            out_shape=result,
            in_specs=[vmem],
            out_specs=hbm,
            scratch_shapes=[dma((n, 4))],
            compiler_params=pltpu.CompilerParams(vmem_limit_bytes=1024 * 1024),
            cost_estimate=pl.CostEstimate(flops=10**10, bytes_accessed=2 * n * d * ff, transcendentals=0),
            name="copy_out",
        )(most)
        out = add(2, out, turn_mine, turn_got, turn_other, turn_got_other)
        late_got_other = lax.ppermute(late_got, "dp", across)
        return add(1, out, late_mine, late_got, late_other, late_got_other)

    return jax.shard_map(
        sums, mesh=mesh, in_specs=(P(("rep", "dp")),) * 2, out_specs=P("rep"), check_vma=False
    )
```

```python
import functools

import jax
import jax.numpy as jnp
from jax import lax
from jax.experimental import pallas as pl
from jax.experimental.pallas import tpu as pltpu
from jax.sharding import PartitionSpec as P


MESH = pl.DeviceIdType.MESH
COLS = 256
STRIP = 128
G_SLOTS = 3
LAG = 4
P_RING = 4
X_RING = 12
SPLIT = 4


def kernel(
    a_ref, g_ref, out_ref, got, mine0, other0, mine1, other1, mine2, other2,
    at, raw, gs, p_send, acc, s_own, s_recv,
    a_sem, g_sem, ps_sem, p0_sem, pr_sem, xs_sem, xr_sem, rs_sem, rr_sem, o_sem,
):
    n_mat, rows, cols = out_ref.shape
    half = rows // 2
    size = half // 2
    per = cols // COLS
    panels = n_mat * per
    turn = panels - 3
    strips = rows // STRIP
    pairs = strips // 2
    rest = STRIP // 2

    me = lax.axis_index("dp")
    core = lax.rem(me, 2)
    sibling = me + 1 - 2 * core
    peer = lax.rem(me + 2, 4)
    own = pl.multiple_of(core * half, half)
    other = pl.multiple_of((1 - core) * half, half)

    def load_strip(n, r, slot):
        c = pl.multiple_of(r * STRIP, STRIP)
        return pltpu.make_async_copy(a_ref.at[0, n, :, pl.ds(c, STRIP)], raw.at[slot], a_sem.at[slot])

    def load_panel(p):
        c = pl.multiple_of(lax.rem(p, per) * COLS, COLS)
        slot = lax.rem(p, G_SLOTS)
        return pltpu.make_async_copy(g_ref.at[0, p // per, :, pl.ds(c, COLS)], gs.at[slot], g_sem.at[slot])

    def tile(p, first, n):
        c = pl.multiple_of(lax.rem(p, per) * COLS, COLS)
        return out_ref.at[p // per, pl.ds(first, n), pl.ds(c, COLS)]

    def remote(src, dst, send, recv, to):
        return pltpu.make_async_remote_copy(
            src_ref=src, dst_ref=dst, send_sem=send, recv_sem=recv,
            device_id={"dp": to}, device_id_type=MESH)

    def exchange(p, lo, n, recv):
        return remote(s_own.at[p, pl.ds(lo, n)], s_recv.at[p, pl.ds(lo, n)], xs_sem, recv, peer)

    def chip_sum(p, lo, n, mine):
        got = tile(p, own + lo, n)[...].astype(jnp.float32)
        s_own[p, pl.ds(lo, n)] = (mine[...] + got).astype(s_own.dtype)

    def flip(r):
        at[pl.ds(pl.multiple_of(r * STRIP, STRIP), STRIP)] = raw[r].T

    def dot(first, n, slot):
        return lax.dot_general(
            at[pl.ds(first, n)], gs[slot], (((1,), (0,)), ((), ())), preferred_element_type=jnp.float32)

    def strip(k):
        h = core + (1 - 2 * core) * (1 - lax.rem(k, 2))
        mid = k // (2 * pairs)
        return (1 - mid) * (h * (pairs + 1) + k // 2) + mid * pairs, h

    def lower(h, i):
        return pl.multiple_of(h * rest + i * STRIP, rest)

    load_strip(0, *[strip(0)[0]] * 2).start()
    load_panel(0).start()

    def load(k, c):
        load_strip(0, *[strip(k)[0]] * 2).start()
        return c

    lax.fori_loop(1, strips, load, 0)
    for p in range(1, G_SLOTS):
        load_panel(p).start()

    barrier = pltpu.get_barrier_semaphore()
    for d in (sibling, peer):
        pl.semaphore_signal(barrier, inc=1, device_id={"dp": d}, device_id_type=MESH)

    def send_strip(lo, n, i):
        return remote(p_send.at[0, pl.ds(lo, n)], tile(0, other + lo, n), ps_sem.at[0], p0_sem.at[i], sibling)

    def take_strip(lo, n, i):
        remote(p_send.at[0, pl.ds(lo, n)], tile(0, own + lo, n), ps_sem.at[0], p0_sem.at[i], sibling).wait_recv()
        chip_sum(0, lo, n, acc.at[pl.ds(lo, n)])
        exchange(0, lo, n, xr_sem.at[0]).start()

    flat = acc.at[pl.ds(half, STRIP)]

    def fill(k, carry):
        r, h = strip(k)
        i = k // 2

        @pl.when(k == 0)
        def _():
            load_panel(0).wait()

        load_strip(0, r, r).wait()
        flip(r)
        flat[...] = dot(pl.multiple_of(r * STRIP, STRIP), STRIP, 0)

        @pl.when((lax.rem(k, 2) == 0) & (k < 2 * pairs))
        def _():
            lo = lower(h, i)
            p_send[0, pl.ds(lo, STRIP)] = flat[...].astype(p_send.dtype)

            @pl.when(k == 0)
            def _():
                pl.semaphore_wait(barrier, 2)

            send_strip(lo, STRIP, i).start()

        @pl.when(lax.rem(k, 2) == 1)
        def _():
            acc[pl.ds(lower(h, i), STRIP)] = flat[...]

        @pl.when(k == 2 * pairs)
        def _():
            lo = pl.multiple_of(core * pairs * STRIP, rest)
            theirs = pl.multiple_of((1 - core) * rest, rest)
            p_send[0, pl.ds(lo, rest)] = flat[pl.ds(theirs, rest)].astype(p_send.dtype)
            send_strip(lo, rest, pairs).start()
            mine = pl.multiple_of(core * rest, rest)
            acc[pl.ds(pl.multiple_of((1 - core) * pairs * STRIP, rest), rest)] = flat[pl.ds(mine, rest)]

        @pl.when((lax.rem(k, 2) == 0) & (k >= 2))
        def _():
            take_strip(lower(core, i - 1), STRIP, i - 1)

        return carry

    lax.fori_loop(0, strips, fill, 0)
    take_strip(pl.multiple_of((1 - core) * pairs * STRIP, rest), rest, pairs)
    load_panel(G_SLOTS).start()

    def spot(k):
        return k // 2, pl.multiple_of(lax.rem(k, 2) * size, size)

    def send_partial(k):
        p, lo = spot(k)
        slot = lax.rem(k, 2)
        return remote(p_send.at[slot, pl.ds(0, size)], tile(p, other + lo, size), ps_sem.at[slot], pr_sem.at[lax.rem(k, P_RING)], sibling)

    def finish(k):
        p, lo = spot(k)
        remote(p_send.at[0, pl.ds(0, size)], tile(p, own + lo, size), ps_sem.at[0], pr_sem.at[lax.rem(k, P_RING)], sibling).wait_recv()
        chip_sum(p, lo, size, acc.at[pl.ds(size, size)])
        here = pl.ds(lo, size)
        for i, (mine, other) in enumerate(((mine0, other0), (mine1, other1), (mine2, other2))):

            @pl.when(p == turn + i)
            def _(mine=mine, other=other):
                mine[here] = s_own[p, here]
                remote(mine.at[here], other.at[here], rs_sem, rr_sem if i else o_sem, sibling).start()

    def arrival(p):
        return xr_sem.at[lax.rem(p, X_RING)]

    def leave(k):
        p, lo = spot(k)

        @pl.when(p < SPLIT)
        def _():
            exchange(p, lo, size, arrival(p)).start()

        @pl.when((lo > 0) & (p >= SPLIT) & (p < turn))
        def _():
            exchange(p, 0, half, arrival(p)).start()

        @pl.when((lo > 0) & (p == turn) & (core == 1))
        def _():
            alone(s_own.at[turn], 0).start()

        @pl.when((lo > 0) & (p == turn))
        def _():
            remote(mine0, other0, rs_sem, o_sem, sibling).wait_recv()

        @pl.when((lo > 0) & (p == turn) & (core == 1))
        def _():
            alone(other0, 1).start()

    def alone(src, i):
        return remote(src, got.at[i], xs_sem, xr_sem.at[turn % X_RING], peer)

    def combine(p):
        exchange(p, 0, half, arrival(p)).wait_recv()

        def one(b, c):
            lo = pl.multiple_of(b * size, size)
            both = s_own[p, pl.ds(lo, size)].astype(jnp.float32) + s_recv[p, pl.ds(lo, size)].astype(jnp.float32)
            here = tile(p, own + lo, size)
            here[...] = both.astype(out_ref.dtype)
            remote(here, here, rs_sem, rr_sem, sibling).start()
            return c

        lax.fori_loop(0, 2, one, 0)

    def step(q, carry):
        k, t = q // 2, lax.rem(q, 2)
        p, b = k // 2, lax.rem(k, 2)
        n, j = p // per, lax.rem(p, per)

        @pl.when((b == 0) & (t == 0))
        def _():
            load_panel(p).wait()

            @pl.when(j == 0)
            def _():
                def turn(r, c):
                    load_strip(0, r, r).wait()
                    flip(r)
                    return c

                lax.fori_loop(0, strips, turn, 0)

            @pl.when((j == 1) & (n < n_mat - 1))
            def _():
                def more(r, c):
                    load_strip(n + 1, r, r).start()
                    return c

                lax.fori_loop(0, strips, more, 0)

        h = core + (1 - 2 * core) * (1 - t)
        acc[pl.ds(pl.multiple_of(t * size, size), size)] = dot(
            pl.multiple_of((2 * h + b) * size, size), size, lax.rem(p, G_SLOTS))

        @pl.when(t == 0)
        def _():
            @pl.when(k == 2)
            def _():
                send_strip(0, half, 0).wait_send()

            @pl.when(k >= 4)
            def _():
                send_partial(k - 2).wait_send()

            p_send[lax.rem(k, 2), pl.ds(0, size)] = acc[pl.ds(0, size)].astype(p_send.dtype)

        @pl.when(t == 0)
        def _():
            send_partial(k).start()

        @pl.when((t == 1) & (b == 1) & (p + G_SLOTS < panels))
        def _():
            load_panel(p + G_SLOTS).start()

        @pl.when(t == 1)
        def _():
            finish(k)
            leave(k)

        @pl.when((t == 1) & (b == 1) & (p >= LAG) & (p < turn + LAG))
        def _():
            combine(p - LAG)

        return carry

    lax.fori_loop(4, 4 * panels, step, 0)

    def drain(p, carry):
        combine(p)
        return carry

    lax.fori_loop(min(panels - LAG, turn), turn, drain, 0)

    for k in (2 * panels - 2, 2 * panels - 1):
        send_partial(k).wait_send()

    remote(s_own.at[pl.ds(0, turn)], s_recv.at[pl.ds(0, turn)], xs_sem, rr_sem, peer).wait_send()
    remote(s_own, s_recv, rs_sem, rr_sem, sibling).wait_send()
    rest_of = pl.ds(0, panels - 1)
    remote(s_own.at[rest_of], s_recv.at[rest_of], rs_sem, rr_sem, sibling).wait_recv()

    @pl.when(core == 1)
    def _():
        remote(got, got, xs_sem, xr_sem.at[turn % X_RING], peer).wait()


def copy_out(x_ref, o_ref, sem):
    n, rows, _ = x_ref.shape
    size = rows // 4
    copies = []
    for i in range(n):
        for j in range(4):
            part = (i, pl.ds(j * size, size))
            copies.append(pltpu.make_async_copy(x_ref.at[part], o_ref.at[part], sem.at[i, j]))
    for c in copies:
        c.start()
    for c in copies:
        c.wait()


def add_panel(back, so_far, mine, got, other, got_other, o_ref, buf, sem):
    n_mat, rows, cols = o_ref.shape
    half = rows // 2
    per = cols // COLS
    n, j = divmod(n_mat * per - back, per)
    core = lax.rem(lax.axis_index("dp"), 2)
    copies = []
    for h, (ours, theirs) in enumerate(((mine, got), (other, got_other))):
        buf[h] = (ours[...].astype(jnp.float32) + theirs[...].astype(jnp.float32)).astype(buf.dtype)
        first = pl.multiple_of((core + (1 - 2 * core) * h) * half, half)
        there = o_ref.at[n, pl.ds(first, half), pl.ds(j * COLS, COLS)]
        copies.append(pltpu.make_async_copy(buf.at[h], there, sem.at[h]))
        copies[-1].start()
    for c in copies:
        c.wait()


def add_two(so_far, mine0, other0, mine1, other1, got, got_other, late, late_other, o_ref, buf, sem):
    n_mat, rows, cols = o_ref.shape
    half = rows // 2
    per = cols // COLS
    core = lax.rem(lax.axis_index("dp"), 2)

    def put(to, ours, theirs):
        to[...] = (ours[...].astype(jnp.float32) + theirs[...].astype(jnp.float32)).astype(buf.dtype)

    def copy(i, h):
        n, j = divmod(n_mat * per - 3 + i, per)
        row = pl.multiple_of((core + (1 - 2 * core) * h) * half, half)
        there = o_ref.at[n, pl.ds(row, half), pl.ds(j * COLS, COLS)]
        return pltpu.make_async_copy(buf.at[i, h], there, sem.at[i, h])

    put(buf.at[1, 0], mine1, late)
    put(buf.at[1, 1], other1, late_other)

    @pl.when(core == 0)
    def _():
        put(buf.at[0, 0], mine0, got_other.at[1])
        put(buf.at[0, 1], other0, got_other.at[0])

    @pl.when(core == 1)
    def _():
        put(buf.at[0, 0], mine0, got.at[0])
        put(buf.at[0, 1], other0, got.at[1])

    for i in range(2):
        for h in range(2):
            copy(i, h).start()
    for i in range(2):
        for h in range(2):
            copy(i, h).wait()


def solution(mesh):
    def sums(a, g):
        _, n, tokens, d = a.shape
        ff = g.shape[-1]
        half, panels, strips = d // 2, n * ff // COLS, d // STRIP
        dma = pltpu.SemaphoreType.DMA
        block = (half, COLS)
        cross, across = [(0, 2), (2, 0), (1, 3), (3, 1)], [(0, 1), (1, 0), (2, 3), (3, 2)]
        vmem, hbm = pl.BlockSpec(memory_space=pltpu.VMEM), pl.BlockSpec(memory_space=pltpu.HBM)
        result = jax.ShapeDtypeStruct((n, d, ff), jnp.bfloat16)
        most, got, *late = pl.pallas_call(
            kernel,
            out_shape=(pltpu.VMEM((n, d, ff), jnp.bfloat16), pltpu.VMEM((2, *block), jnp.bfloat16), *[pltpu.VMEM(block, jnp.bfloat16)] * 6),
            in_specs=[pl.BlockSpec(memory_space=pl.ANY)] * 2,
            out_specs=(vmem,) * 8,
            scratch_shapes=[
                pltpu.VMEM((d, tokens), jnp.bfloat16),
                pltpu.VMEM((strips, tokens, STRIP), jnp.bfloat16),
                pltpu.VMEM((G_SLOTS, tokens, COLS), jnp.bfloat16),
                pltpu.VMEM((2, half, COLS), jnp.bfloat16),
                pltpu.VMEM((half + STRIP, COLS), jnp.float32),
                pltpu.VMEM((panels, half, COLS), jnp.bfloat16),
                pltpu.VMEM((panels, half, COLS), jnp.bfloat16),
                dma((strips,)), dma((G_SLOTS,)), dma((2,)), dma((strips // 2 + 1,)), dma((P_RING,)),
                dma, dma((X_RING,)), dma, dma, dma,
            ],
            compiler_params=pltpu.CompilerParams(
                collective_id=0, has_side_effects=True, vmem_limit_bytes=46 * 1024 * 1024
            ),
            name="sums",
        )(a, g)
        mine, other = late[::2], late[1::2]

        def local(body, n_terms, bufs, sems):
            return pl.pallas_call(
                body,
                out_shape=result,
                in_specs=[hbm] + [vmem] * n_terms,
                out_specs=hbm,
                scratch_shapes=[pltpu.VMEM((*bufs, *block), jnp.bfloat16), dma(sems)],
                input_output_aliases={0: 0},
                compiler_params=pltpu.CompilerParams(vmem_limit_bytes=4 * 1024 * 1024),
                name="add",
            )

        late0 = lax.ppermute(mine[1], "dp", cross)
        late1 = lax.ppermute(mine[2], "dp", cross)
        out = pl.pallas_call(
            copy_out,
            out_shape=result,
            in_specs=[vmem],
            out_specs=hbm,
            scratch_shapes=[dma((n, 4))],
            compiler_params=pltpu.CompilerParams(vmem_limit_bytes=1024 * 1024),
            cost_estimate=pl.CostEstimate(flops=10**10, bytes_accessed=2 * n * d * ff, transcendentals=0),
            name="copy_out",
        )(most)
        got_other = lax.ppermute(got, "dp", across)
        late0_other = lax.ppermute(late0, "dp", across)
        late1_other = lax.ppermute(late1, "dp", across)
        out = local(add_two, 8, (2, 2), (2, 2))(
            out, mine[0], other[0], mine[1], other[1], got, got_other, late0, late0_other
        )
        return local(functools.partial(add_panel, 1), 4, (2,), (2,))(out, mine[2], late1, other[2], late1_other)

    return jax.shard_map(
        sums, mesh=mesh, in_specs=(P(("rep", "dp")),) * 2, out_specs=P("rep"), check_vma=False
    )
```
